32 devices in a mesh: tm: 8 (over z, x), tp: 4 (over y, core).
Axes of the slice: x: 2, y: 2, z: 4, core: 2. Of those that a mesh axis runs over, the one named last changes fastest.
Arguments:
- trajectory: float32 [16, 128, 3072], P('tm', None, 'tp'), may hold values from -6 to 6
- offset: int32 [1], replicated, may hold values from 0 to 15
- step_gaps: int32 [16], P('tm'), may hold values from 1 to 4, as said below
- qkv_weight: bfloat16 [3072, 3, 3072], P(None, None, 'tp')
- out_weight: bfloat16 [3072, 3072], P('tp'), may hold values from -4 to 4
- mod_weight: bfloat16 [256, 3, 3072], P(None, None, 'tp'), may hold values from -0.375 to 0.375
Outputs:
- advanced: float32 [16, 128, 3072], P('tm', None, 'tp')
The draws below stay inside these ranges and needn't reach their ends.
Inputs may be any that keep to these rules, and one draw needn't show every extreme that they name: `step_gaps`: in aligned blocks of 2 timesteps, the gaps of block b sum to an even number for even b and to an odd number for odd b.
All inputs are finite; a program needn't handle non-finite values.
Results may differ from the reference program's by a relative error of at most 0.007.
Values may be sent and summed in bfloat16 or wider, within the bound.
A program may use at most 128 MiB of HBM per device.

```python
import math
import jax
import jax.numpy as jnp
from jax import lax

D = 3072
HEADS = 24
HD = 128
FREQ = 256
TOK = 128
STEP_DEV = 2
ITERS = 2
TIME = 16
SCHED = 80


def draw_step_gaps(key, part):
    key_gaps = jax.random.fold_in(key, 37)
    gaps = jax.random.randint(key_gaps, (TIME,), 1, 5, dtype=jnp.int32)
    blocks = gaps.reshape(TIME // STEP_DEV, STEP_DEV)
    totals = jnp.sum(blocks, 1)
    parity = jnp.arange(TIME // STEP_DEV, dtype=jnp.int32) % 2
    wrong = totals % 2 != parity
    last_gap = blocks[:, -1]
    fixed_gap = jnp.where(last_gap < 4, last_gap + 1, 3)
    new_last = jnp.where(wrong, fixed_gap, last_gap)
    blocks = jnp.concatenate([blocks[:, :-1], new_last[:, None]], 1)
    return blocks.reshape(TIME).astype(jnp.int32)


def draw_qkv_weight(key, part):
    key_norm = jax.random.fold_in(key, 11)
    drawn = jax.random.normal(key_norm, (D, 3, D), jnp.float32) / math.sqrt(D)
    return drawn.astype(jnp.bfloat16)


def block_scale(stream_key, shape, cuts, low, top_value):
    factor_of, own = 1.0, jax.random.fold_in(stream_key, 6)
    for position, shards_of in cuts:
        steps = jnp.exp(jax.random.uniform(jax.random.fold_in(own, position), (shards_of,), jnp.float32, low / len(cuts), top_value / len(cuts)))
        factor_of = factor_of * jnp.repeat(steps, shape[position] // shards_of).reshape([-1 if axis == position else 1 for axis in range(len(shape))])
    return factor_of


def centred(rng, dims, scale, limit, cuts=(), kind=jnp.bfloat16):
    level = block_scale(rng, dims, cuts, -0.22, 0.18) if cuts else 1.0
    result = jax.random.normal(rng, dims, jnp.float32) * scale * level
    return jnp.minimum(jnp.maximum(result, -limit), limit).astype(kind)


def setup_inputs(seed: int = 0) -> dict:
    seeds = jax.random.split(jax.random.key(seed), 7)
    return {
        "trajectory": centred(seeds[0], (TIME, TOK, D), 1.0, 6.0, ((0, 8), (2, 4)), jnp.float32),
        "offset": jax.random.randint(seeds[1], (1,), 0, TIME).astype(jnp.int32),
        "step_gaps": draw_step_gaps(jax.random.fold_in(seeds[6], 71), 0),
        "qkv_weight": draw_qkv_weight(jax.random.fold_in(seeds[6], 71), 0),
        "out_weight": centred(seeds[4], (D, D), 0.25, 4.0, ((0, 4),)),
        "mod_weight": centred(seeds[5], (FREQ, 3, D), FREQ ** -0.5, 0.375, ((2, 4),)),
    }


def noise_levels(offset, step_gaps):
    before = jnp.cumsum(step_gaps) - step_gaps
    levels = (offset[0] + before).astype(jnp.float32)
    sigma = 1.0 - levels / SCHED
    step_size = step_gaps.astype(jnp.float32) / SCHED
    return (sigma, step_size)

def embedding(sigma):
    half_freq = FREQ // 2
    frequencies = jnp.exp(-math.log(10000.0) * jnp.arange(half_freq, dtype=jnp.float32) / half_freq)
    angles = 1000.0 * sigma[:, None] * frequencies[None, :]
    return jnp.concatenate([jnp.cos(angles), jnp.sin(angles)], -1).astype(jnp.bfloat16)

def one_head(triple):
    queries, key_rows, values = triple
    scores = jnp.dot(queries, key_rows.T, preferred_element_type=jnp.float32) * (1.0 / math.sqrt(HD))
    row_max = lax.optimization_barrier(jnp.max(scores, -1, keepdims=True))
    weights_exp = jnp.exp(scores - row_max)
    probs = (weights_exp / lax.optimization_barrier(jnp.sum(weights_exp, -1, keepdims=True))).astype(jnp.bfloat16)
    return jnp.dot(probs, values, preferred_element_type=jnp.float32).astype(jnp.bfloat16)

def drift_of(state, modulation, qkv_weight, out_weight):
    row_total = lax.optimization_barrier(jnp.sum(state, -1, keepdims=True))
    row_squares = lax.optimization_barrier(jnp.sum(state * state, -1, keepdims=True))
    row_mean = row_total / D
    variance = row_squares / D - row_mean * row_mean
    inv_std = lax.rsqrt(variance + 1e-06)
    normed = ((state - row_mean) * inv_std * (1.0 + modulation[1]) + modulation[0]).astype(jnp.bfloat16)
    projected = jnp.dot(normed, qkv_weight.reshape(D, 3 * D), preferred_element_type=jnp.float32)
    projected = projected.astype(jnp.bfloat16).reshape(TOK, 3, HEADS, HD)
    per_head = jnp.transpose(projected, (1, 2, 0, 3))
    attended = lax.map(one_head, (per_head[0], per_head[1], per_head[2]))
    attended = jnp.transpose(attended, (1, 0, 2)).reshape(TOK, D)
    head_out = jnp.dot(attended, out_weight, preferred_element_type=jnp.float32)
    return modulation[2] * head_out

def reference(trajectory, offset, step_gaps, qkv_weight, out_weight, mod_weight):
    sigma, step_size = noise_levels(offset, step_gaps)
    embed_rows = embedding(sigma)
    modulation = jnp.dot(embed_rows, mod_weight.reshape(FREQ, 3 * D), preferred_element_type=jnp.float32).reshape(TIME, 3, D)
    start_point = trajectory[0]
    states = trajectory
    points = trajectory
    for sweep in range(ITERS):
        drifts = lax.map(lambda pair: drift_of(pair[0], pair[1], qkv_weight, out_weight), (states, modulation))
        increments = -step_size[:, None, None] * drifts
        points = start_point[None] + jnp.cumsum(increments, 0)
        states = jnp.concatenate([start_point[None], points[:-1]], 0)
    return points
```

```python
import functools
import math

import jax
import jax.numpy as jnp
from jax import lax
from jax.experimental import pallas as pl
from jax.experimental.pallas import tpu as pltpu
from jax.sharding import PartitionSpec as P

HD = 128
FREQ = 256
ITERS = 2
F32 = jnp.float32
BF16 = jnp.bfloat16
MESH = pl.DeviceIdType.MESH


def level_table(level_count):
    rows = -(-level_count // 128) * 128
    sigma = 1.0 - jnp.arange(rows, dtype=jnp.int32).astype(F32) / level_count
    half_freq = FREQ // 2
    frequencies = jnp.exp(-math.log(10000.0) * jnp.arange(half_freq, dtype=F32) / half_freq)
    angles = 1000.0 * sigma[:, None] * frequencies[None, :]
    return jnp.concatenate([jnp.cos(angles), jnp.sin(angles)], -1).astype(BF16)


def kernel(
    tm, tp, steps, tok, col,
    offset, gaps, traj_hbm, table_hbm, mod_hbm, qkv_hbm, out_hbm, result,
    traj, table, mod_w, qkv_w, out_w, mods,
    gap_buf, stat_buf, normed, acc, attended,
    rs_part, rs_cross, inc, tot, pair_send, pair_recv, chain_send, chain_recv,
    last_send, last_recv, prefix, start, start_b,
    load_sem, gap_send_sem, gap_recv_sem, stat_sem, ag_sem, rs_sem, scan_sem,
    chain_sem, start_send_sem, start_recv_sem,
):
    k = lax.axis_index("tm")
    j = lax.axis_index("tp")
    rows = steps * tok
    width = tp * col
    half = col // 2
    groups = tp // 2
    pairs = tm // 2
    core = lax.rem(j, 2)
    group = lax.div(j, 2)
    side = lax.rem(k, 2)
    link = lax.div(k, 2)
    partner = group * 2 + (1 - core)
    neighbour = link * 2 + (1 - side)

    loads = [
        pltpu.make_async_copy(src, dst, load_sem.at[n])
        for n, (src, dst) in enumerate(
            ((traj_hbm, traj), (table_hbm, table), (mod_hbm, mod_w), (qkv_hbm, qkv_w), (out_hbm, out_w))
        )
    ]
    for load in loads:
        load.start()

    barrier = pltpu.get_barrier_semaphore()
    for d in range(1, tp):
        pl.semaphore_signal(
            barrier, inc=1, device_id=(k, lax.rem(j + d, tp)), device_id_type=MESH
        )
    for d in range(1, tm):
        pl.semaphore_signal(
            barrier, inc=1, device_id=(lax.rem(k + d, tm), j), device_id_type=MESH
        )

    def send(src, dst, send_sem, recv_sem, to_k, to_j):
        return pltpu.make_async_remote_copy(
            src_ref=src, dst_ref=dst, send_sem=send_sem, recv_sem=recv_sem,
            device_id=(to_k, to_j), device_id_type=MESH,
        )

    own_total = gaps[0]
    for s in range(1, steps):
        own_total = own_total + gaps[s]
    gap_buf[0] = jnp.full((8, 128), own_total, jnp.int32)
    loads[0].wait()

    def stats_of(sweep):
        x = traj[...].reshape(rows, col)
        total = jnp.sum(x, -1, keepdims=True)
        squares = jnp.sum(x * x, -1, keepdims=True)
        lane = lax.broadcasted_iota(jnp.int32, (rows, 128), 1)
        both = jnp.where(lane == 0, total, jnp.where(lane == 1, squares, 0.0))
        stat_buf[sweep, 0] = jnp.transpose(both)[0:8]

    stats_of(0)
    start_b[0] = traj[0].astype(BF16)
    pl.semaphore_wait(barrier, tp - 1 + tm - 1)

    def stat_copy(sweep, d):
        return send(
            stat_buf.at[sweep, 0], stat_buf.at[sweep, d],
            stat_sem.at[sweep, 0, d], stat_sem.at[sweep, 1, d], k, lax.rem(j + d, tp),
        )

    def gap_copy(d):
        return send(
            gap_buf.at[0], gap_buf.at[d], gap_send_sem.at[d], gap_recv_sem.at[d],
            lax.rem(k + d, tm), j,
        )

    def start_copy(d):
        return send(start_b.at[0], start_b.at[1], start_send_sem.at[d], start_recv_sem, d, j)

    for d in range(1, tm):
        gap_copy(d).start()
    for d in range(1, tp):
        stat_copy(0, d).start()

    @pl.when(k == 0)
    def _():
        for d in range(1, tm):
            start_copy(d).start()

    before = jnp.full((8, 128), offset[0], jnp.int32)
    for d in range(1, tm):
        gap_copy(d).wait_recv()
        before = before + jnp.where(k >= d, gap_buf[d], 0)
    row = lax.broadcasted_iota(jnp.int32, (8, 128), 0)
    for s in range(steps):
        before = before + jnp.where(row > s, gaps[s], 0)
    loads[1].wait()
    table_rows = table.shape[0]
    levels = jnp.concatenate([before] * (table_rows // 128), -1)
    pick = (lax.broadcasted_iota(jnp.int32, (8, table_rows), 1) == levels).astype(F32).astype(BF16)
    embed = jnp.dot(pick, table[...], preferred_element_type=F32).astype(BF16)
    loads[2].wait()
    for part in range(3):
        mods[part] = jnp.dot(embed, mod_w[part], preferred_element_type=F32)

    def ag_copy(sweep, kind, g, s):
        sems = (ag_sem.at[sweep, 0, kind, g, s], ag_sem.at[sweep, 1, kind, g, s])
        if kind == 0:
            return send(normed.at[sweep, 0, s], normed.at[sweep, 1, s], *sems, k, partner)
        if kind == 1:
            there = lax.rem(group + g, groups) * 2 + core
            return send(normed.at[sweep, 0, s], normed.at[sweep, 2 * g, s], *sems, k, there)
        return send(normed.at[sweep, 2 * g, s], normed.at[sweep, 2 * g + 1, s], *sems, k, partner)

    def part_copy(sweep, g):
        return send(
            rs_part.at[sweep, 0, g], rs_part.at[sweep, 1, g],
            rs_sem.at[sweep, 0, 0, g], rs_sem.at[sweep, 1, 0, g], k, partner,
        )

    def cross_copy(sweep, g):
        there = lax.rem(group + g, groups) * 2 + core
        return send(
            rs_cross.at[sweep, 0, g - 1], rs_cross.at[sweep, 1, g - 1],
            rs_sem.at[sweep, 0, 1, g], rs_sem.at[sweep, 1, 1, g], k, there,
        )

    def pair_copy(sweep):
        return send(
            pair_send.at[sweep], pair_recv.at[sweep],
            scan_sem.at[sweep, 0, 0], scan_sem.at[sweep, 1, 0], neighbour, j,
        )

    def last_copy(sweep, c):
        return send(
            last_send.at[sweep, c], last_recv.at[sweep, c],
            chain_sem.at[sweep, 2, c], chain_sem.at[sweep, 3, c], neighbour, j,
        )

    def chain_copy(sweep, c):
        return send(
            chain_send.at[sweep, c], chain_recv.at[sweep, c],
            chain_sem.at[sweep, 0, c], chain_sem.at[sweep, 1, c], lax.rem(k + 2, tm), j,
        )

    chunks = chain_send.shape[1]
    piece = tok // chunks

    for sweep in range(ITERS):
        if sweep > 0:
            stats_of(sweep)
            for d in range(1, tp):
                stat_copy(sweep, d).start()
        stats = stat_buf[sweep, 0]
        for d in range(1, tp):
            stat_copy(sweep, d).wait_recv()
            stats = stats + stat_buf[sweep, d]
        stats = jnp.transpose(
            jnp.concatenate([stats, jnp.zeros((120, rows), F32)], 0)
        )
        row_mean = stats[:, 0:1] / width
        variance = stats[:, 1:2] / width - row_mean * row_mean
        inv_std = lax.rsqrt(variance + 1e-06)
        for s in range(steps):
            part = slice(s * tok, (s + 1) * tok)
            normed[sweep, 0, s] = (
                (traj[s] - row_mean[part]) * inv_std[part] * (1.0 + mods[1, s : s + 1])
                + mods[0, s : s + 1]
            ).astype(BF16)
            for g in range(1, groups):
                ag_copy(sweep, 1, g, s).start()
            ag_copy(sweep, 0, 0, s).start()

        if sweep == 0:
            loads[3].wait()

        def project(slot, owner):
            block = normed[sweep, slot].reshape(rows, col)
            at = pl.multiple_of(owner * col, col)

            def one(part, carry):
                product = jnp.dot(block, qkv_w[part, pl.ds(at, col), :], preferred_element_type=F32)
                if slot == 0:
                    acc[part] = product
                else:
                    acc[part] = acc[part] + product
                return carry

            lax.fori_loop(0, 3, one, 0)

        project(0, j)
        for s in range(steps):
            ag_copy(sweep, 0, 0, s).wait_recv()
        project(1, partner)
        for g in range(1, groups):
            for s in range(steps):
                ag_copy(sweep, 1, g, s).wait_recv()
                ag_copy(sweep, 2, g, s).start()
            owner = lax.rem(group + groups - g, groups) * 2
            project(2 * g, owner + core)
            for s in range(steps):
                ag_copy(sweep, 2, g, s).wait_recv()
            project(2 * g + 1, owner + 1 - core)

        def attend(s, carry):
            at = pl.ds(pl.multiple_of(s * tok, tok), tok)
            for head in range(col // HD):
                lanes = slice(head * HD, (head + 1) * HD)
                queries = acc[0, at, lanes].astype(BF16)
                key_rows = acc[1, at, lanes].astype(BF16)
                values = acc[2, at, lanes].astype(BF16)
                scores = lax.dot_general(
                    queries, key_rows, (((1,), (1,)), ((), ())), preferred_element_type=F32
                ) * (1.0 / math.sqrt(HD))
                weights_exp = jnp.exp(scores - jnp.max(scores, -1, keepdims=True))
                probs = (weights_exp / jnp.sum(weights_exp, -1, keepdims=True)).astype(BF16)
                attended[at, lanes] = jnp.dot(
                    probs, values, preferred_element_type=F32
                ).astype(BF16)
            return carry

        lax.fori_loop(0, steps, attend, 0)
        if sweep == 0:
            loads[4].wait()

        def head_out(dest):
            at = pl.ds(pl.multiple_of(dest * col, col), col)
            return jnp.dot(attended[...], out_w[:, at], preferred_element_type=F32)

        for g in list(range(1, groups)) + [0]:
            there = lax.rem(group + g, groups) * 2
            rs_part[sweep, 0, g] = head_out(there + 1 - core).astype(BF16)
            part_copy(sweep, g).start()
            mine = head_out(there + core)
            if g > 0:
                part_copy(sweep, g).wait_recv()
                rs_cross[sweep, 0, g - 1] = (mine + rs_part[sweep, 1, g].astype(F32)).astype(BF16)
                cross_copy(sweep, g).start()
            else:
                inc[...] = mine.reshape(steps, tok, col)
        part_copy(sweep, 0).wait_recv()
        share = inc[...].reshape(rows, col) + rs_part[sweep, 1, 0].astype(F32)
        for g in range(1, groups):
            cross_copy(sweep, g).wait_recv()
            share = share + rs_cross[sweep, 1, g - 1].astype(F32)

        running = jnp.zeros((tok, col), F32)
        for s in range(steps):
            size = gaps[s].astype(F32) / (5 * steps * tm)
            running = running - size * (mods[2, s : s + 1] * share[s * tok : (s + 1) * tok])
            inc[s] = running
        for h in range(2):
            tot[h] = running[:, h * half : (h + 1) * half]
        pair_send[sweep] = tot[1 - side].astype(BF16)
        pair_copy(sweep).start()

        @pl.when(link == 0)
        def _():
            chain_recv[sweep] = jnp.zeros_like(chain_recv[sweep])

        pair_copy(sweep).wait_recv()
        first = side == 0
        for c in range(chunks):
            at = slice(c * piece, (c + 1) * piece)
            ours = tot[side, at]
            theirs = pair_recv[sweep, at].astype(F32)

            @pl.when(link > 0)
            def _():
                chain_copy(sweep, c).wait_recv()

            earlier = chain_recv[sweep, c].astype(F32)

            @pl.when(link < pairs - 1)
            def _():
                chain_send[sweep, c] = (earlier + ours + theirs).astype(BF16)
                chain_copy(sweep, c).start()

            last_send[sweep, c] = jnp.where(first, earlier + ours, earlier).astype(BF16)
            last_copy(sweep, c).start()
            prefix[side, at] = jnp.where(first, earlier, earlier + theirs)
        if sweep == 0:
            @pl.when(k > 0)
            def _():
                start_copy(1).wait_recv()
                start[...] = start_b[1].astype(F32)

            @pl.when(k == 0)
            def _():
                start[...] = traj[0]
        for c in range(chunks):
            last_copy(sweep, c).wait_recv()
            prefix[1 - side, c * piece : (c + 1) * piece] = last_recv[sweep, c].astype(F32)
        entry = start[...] + jnp.concatenate([prefix[0], prefix[1]], -1)
        if sweep < ITERS - 1:
            traj[0] = entry
            for s in range(1, steps):
                traj[s] = entry + inc[s - 1]
        else:
            for s in range(steps):
                result[s] = entry + inc[s]

    for d in range(1, tm):
        gap_copy(d).wait_send()

    @pl.when(k == 0)
    def _():
        for d in range(1, tm):
            start_copy(d).wait_send()

    for sweep in range(ITERS):
        for d in range(1, tp):
            stat_copy(sweep, d).wait_send()
        for s in range(steps):
            ag_copy(sweep, 0, 0, s).wait_send()
            for g in range(1, groups):
                ag_copy(sweep, 1, g, s).wait_send()
                ag_copy(sweep, 2, g, s).wait_send()
        for g in range(groups):
            part_copy(sweep, g).wait_send()
            if g > 0:
                cross_copy(sweep, g).wait_send()
        pair_copy(sweep).wait_send()
        for c in range(chunks):
            last_copy(sweep, c).wait_send()

        @pl.when(link < pairs - 1)
        def _():
            for c in range(chunks):
                chain_copy(sweep, c).wait_send()


def solution(mesh):
    tm, tp = mesh.shape["tm"], mesh.shape["tp"]
    chunks = 4

    def body(trajectory, offset, step_gaps, qkv_weight, out_weight, mod_weight):
        steps, tok, col = trajectory.shape
        half, rows, groups = col // 2, steps * tok, tp // 2
        table = level_table(5 * steps * tm)
        qkv = jnp.transpose(qkv_weight, (1, 0, 2))
        mod = jnp.transpose(mod_weight, (1, 0, 2))
        anywhere = pl.BlockSpec(memory_space=pl.ANY)
        smem = pl.BlockSpec(memory_space=pltpu.SMEM)
        vm, dma = pltpu.VMEM, pltpu.SemaphoreType.DMA
        return pl.pallas_call(
            functools.partial(kernel, tm, tp, steps, tok, col),
            out_shape=jax.ShapeDtypeStruct(trajectory.shape, F32),
            in_specs=[smem, smem] + [anywhere] * 5,
            out_specs=pl.BlockSpec(memory_space=pltpu.VMEM),
            scratch_shapes=[
                vm(trajectory.shape, F32),
                vm(table.shape, BF16),
                vm(mod.shape, BF16),
                vm(qkv.shape, BF16),
                vm(out_weight.shape, BF16),
                vm((3, 8, col), F32),
                vm((tm, 8, 128), jnp.int32),
                vm((ITERS, tp, 8, rows), F32),
                vm((ITERS, tp, steps, tok, col), BF16),
                vm((3, rows, col), F32),
                vm((rows, col), BF16),
                vm((ITERS, 2, groups, rows, col), BF16),
                vm((ITERS, 2, max(groups - 1, 1), rows, col), BF16),
                vm((steps, tok, col), F32),
                vm((2, tok, half), F32),
                vm((ITERS, tok, half), BF16),
                vm((ITERS, tok, half), BF16),
                vm((ITERS, chunks, tok // chunks, half), BF16),
                vm((ITERS, chunks, tok // chunks, half), BF16),
                vm((ITERS, chunks, tok // chunks, half), BF16),
                vm((ITERS, chunks, tok // chunks, half), BF16),
                vm((2, tok, half), F32),
                vm((tok, col), F32),
                vm((2, tok, col), BF16),
                dma((5,)),
                dma((tm,)),
                dma((tm,)),
                dma((ITERS, 2, tp)),
                dma((ITERS, 2, 3, groups, steps)),
                dma((ITERS, 2, 2, groups)),
                dma((ITERS, 2, 1)),
                dma((ITERS, 4, chunks)),
                dma((tm,)),
                dma,
            ],
            compiler_params=pltpu.CompilerParams(
                collective_id=0, has_side_effects=True, vmem_limit_bytes=62 * 1024 * 1024
            ),
            name="picard",
        )(offset, step_gaps, trajectory, table, mod, qkv, out_weight)

    placed = (
        P("tm", None, "tp"),
        P(),
        P("tm"),
        P(None, None, "tp"),
        P("tp", None),
        P(None, None, "tp"),
    )
    return jax.shard_map(
        body, mesh=mesh, in_specs=placed, out_specs=P("tm", None, "tp"), check_vma=False
    )
```

```python
import functools
import math

import jax
import jax.numpy as jnp
from jax import lax
from jax.experimental import pallas as pl
from jax.experimental.pallas import tpu as pltpu
from jax.sharding import PartitionSpec as P

HD = 128
FREQ = 256
ITERS = 2
F32 = jnp.float32
BF16 = jnp.bfloat16
MESH = pl.DeviceIdType.MESH


def level_table(level_count):
    rows = -(-level_count // 128) * 128
    sigma = 1.0 - jnp.arange(rows, dtype=jnp.int32).astype(F32) / level_count
    half_freq = FREQ // 2
    frequencies = jnp.exp(-math.log(10000.0) * jnp.arange(half_freq, dtype=F32) / half_freq)
    angles = 1000.0 * sigma[:, None] * frequencies[None, :]
    return jnp.concatenate([jnp.cos(angles), jnp.sin(angles)], -1).astype(BF16)


def kernel(
    tm, tp, steps, tok, col,
    offset, gaps, traj_hbm, table_hbm, mod_hbm, qkv_hbm, out_hbm, result,
    traj, table, mod_w, qkv_w, out_w, mods,
    gap_buf, stat_buf, normed, acc, attended,
    rs_part, rs_cross, mine, inc, chain_send, chain_recv, last_send,
    last_recv, prefix, start, start_b,
    load_sem, gap_send_sem, gap_recv_sem, stat_sem, ag_sem, rs_sem, cross_sem,
    chain_sem, start_send_sem, start_recv_sem,
):
    k = lax.axis_index("tm")
    j = lax.axis_index("tp")
    rows = steps * tok
    width = tp * col
    chunks = chain_send.shape[1]
    groups = tp // 2
    pairs = tm // 2
    core = lax.rem(j, 2)
    group = lax.div(j, 2)
    side = lax.rem(k, 2)
    link = lax.div(k, 2)
    partner = group * 2 + (1 - core)
    neighbour = link * 2 + (1 - side)

    loads = [
        pltpu.make_async_copy(src, dst, load_sem.at[n])
        for n, (src, dst) in enumerate(
            ((traj_hbm, traj), (table_hbm, table), (mod_hbm, mod_w), (qkv_hbm, qkv_w), (out_hbm, out_w))
        )
    ]
    for load in loads:
        load.start()

    barrier = pltpu.get_barrier_semaphore()
    for d in range(1, tp):
        pl.semaphore_signal(
            barrier, inc=1, device_id=(k, lax.rem(j + d, tp)), device_id_type=MESH
        )
    for d in range(1, tm):
        pl.semaphore_signal(
            barrier, inc=1, device_id=(lax.rem(k + d, tm), j), device_id_type=MESH
        )

    def send(src, dst, send_sem, recv_sem, to_k, to_j):
        return pltpu.make_async_remote_copy(
            src_ref=src, dst_ref=dst, send_sem=send_sem, recv_sem=recv_sem,
            device_id=(to_k, to_j), device_id_type=MESH,
        )

    own_total = gaps[0]
    for s in range(1, steps):
        own_total = own_total + gaps[s]
    gap_buf[0] = jnp.full((8, 128), own_total, jnp.int32)
    loads[0].wait()

    def stats_of(sweep):
        x = traj[...].reshape(rows, col)
        total = jnp.sum(x, -1, keepdims=True)
        squares = jnp.sum(x * x, -1, keepdims=True)
        lane = lax.broadcasted_iota(jnp.int32, (rows, 128), 1)
        both = jnp.where(lane == 0, total, jnp.where(lane == 1, squares, 0.0))
        stat_buf[sweep, 0] = jnp.transpose(both)[0:8]

    stats_of(0)
    start_b[0] = traj[0].astype(BF16)
    pl.semaphore_wait(barrier, tp - 1 + tm - 1)

    def stat_copy(sweep, d):
        return send(
            stat_buf.at[sweep, 0], stat_buf.at[sweep, d],
            stat_sem.at[sweep, 0, d], stat_sem.at[sweep, 1, d], k, lax.rem(j + d, tp),
        )

    def gap_copy(d):
        return send(
            gap_buf.at[0], gap_buf.at[d], gap_send_sem.at[d], gap_recv_sem.at[d],
            lax.rem(k + d, tm), j,
        )

    def start_copy(d):
        return send(start_b.at[0], start_b.at[1], start_send_sem.at[d], start_recv_sem, d, j)

    for d in range(1, tm):
        gap_copy(d).start()
    for d in range(1, tp):
        stat_copy(0, d).start()

    @pl.when(k == 0)
    def _():
        for d in range(1, tm):
            start_copy(d).start()

    before = jnp.full((8, 128), offset[0], jnp.int32)
    for d in range(1, tm):
        gap_copy(d).wait_recv()
        before = before + jnp.where(k >= d, gap_buf[d], 0)
    row = lax.broadcasted_iota(jnp.int32, (8, 128), 0)
    for s in range(steps):
        before = before + jnp.where(row > s, gaps[s], 0)
    loads[1].wait()
    table_rows = table.shape[0]
    levels = jnp.concatenate([before] * (table_rows // 128), -1)
    pick = (lax.broadcasted_iota(jnp.int32, (8, table_rows), 1) == levels).astype(F32).astype(BF16)
    embed = jnp.dot(pick, table[...], preferred_element_type=F32).astype(BF16)
    loads[2].wait()
    for part in range(3):
        mods[part] = jnp.dot(embed, mod_w[part], preferred_element_type=F32)

    def ag_copy(sweep, kind, g, s):
        sems = (ag_sem.at[sweep, 0, kind, g, s], ag_sem.at[sweep, 1, kind, g, s])
        if kind == 0:
            return send(normed.at[sweep, 0, s], normed.at[sweep, 1, s], *sems, k, partner)
        if kind == 1:
            there = lax.rem(group + g, groups) * 2 + core
            return send(normed.at[sweep, 0, s], normed.at[sweep, 2 * g, s], *sems, k, there)
        return send(normed.at[sweep, 2 * g, s], normed.at[sweep, 2 * g + 1, s], *sems, k, partner)

    def part_copy(sweep, g, s):
        return send(
            rs_part.at[sweep, 0, g, s], rs_part.at[sweep, 1, g, s],
            rs_sem.at[sweep, 0, g, s], rs_sem.at[sweep, 1, g, s], k, partner,
        )

    def cross_copy(sweep, g, s, c):
        there = lax.rem(group + g, groups) * 2 + core
        return send(
            rs_cross.at[sweep, 0, g - 1, s, c], rs_cross.at[sweep, 1, g - 1, s, c],
            cross_sem.at[sweep, 0, g, s, c], cross_sem.at[sweep, 1, g, s, c], k, there,
        )

    def last_copy(sweep, c):
        return send(
            last_send.at[sweep, c], last_recv.at[sweep, c],
            chain_sem.at[sweep, 2, c], chain_sem.at[sweep, 3, c], neighbour, j,
        )

    def chain_copy(sweep, c):
        return send(
            chain_send.at[sweep, c], chain_recv.at[sweep, c],
            chain_sem.at[sweep, 0, c], chain_sem.at[sweep, 1, c], lax.rem(k + 2, tm), j,
        )

    piece = tok // chunks
    last = steps - 1

    for sweep in range(ITERS):
        if sweep > 0:
            stats_of(sweep)
            for d in range(1, tp):
                stat_copy(sweep, d).start()
        stats = stat_buf[sweep, 0]
        for d in range(1, tp):
            stat_copy(sweep, d).wait_recv()
            stats = stats + stat_buf[sweep, d]
        stats = jnp.transpose(
            jnp.concatenate([stats, jnp.zeros((120, rows), F32)], 0)
        )
        row_mean = stats[:, 0:1] / width
        variance = stats[:, 1:2] / width - row_mean * row_mean
        inv_std = lax.rsqrt(variance + 1e-06)
        for s in range(steps):
            part = slice(s * tok, (s + 1) * tok)
            normed[sweep, 0, s] = (
                (traj[s] - row_mean[part]) * inv_std[part] * (1.0 + mods[1, s : s + 1])
                + mods[0, s : s + 1]
            ).astype(BF16)
            for g in range(1, groups):
                ag_copy(sweep, 1, g, s).start()
            ag_copy(sweep, 0, 0, s).start()

        if sweep == 0:
            loads[3].wait()

        def project(slot, owner, s=None):
            block = normed[sweep, slot].reshape(rows, col) if s is None else normed[sweep, slot, s]
            into = slice(0, rows) if s is None else slice(s * tok, (s + 1) * tok)
            at = pl.multiple_of(owner * col, col)

            def one(part, carry):
                product = jnp.dot(block, qkv_w[part, pl.ds(at, col), :], preferred_element_type=F32)
                if slot == 0:
                    acc[part, into] = product
                else:
                    acc[part, into] = acc[part, into] + product
                return carry

            lax.fori_loop(0, 3, one, 0)

        def attend(s):
            at = slice(s * tok, (s + 1) * tok)
            for head in range(col // HD):
                lanes = slice(head * HD, (head + 1) * HD)
                queries = acc[0, at, lanes].astype(BF16)
                key_rows = acc[1, at, lanes].astype(BF16)
                values = acc[2, at, lanes].astype(BF16)
                scores = lax.dot_general(
                    queries, key_rows, (((1,), (1,)), ((), ())), preferred_element_type=F32
                ) * (1.0 / math.sqrt(HD))
                weights_exp = jnp.exp(scores - jnp.max(scores, -1, keepdims=True))
                probs = (weights_exp / jnp.sum(weights_exp, -1, keepdims=True)).astype(BF16)
                attended[s, :, lanes] = jnp.dot(
                    probs, values, preferred_element_type=F32
                ).astype(BF16)

        def head_out(dest, s):
            at = pl.ds(pl.multiple_of(dest * col, col), col)
            return jnp.dot(attended[s], out_w[:, at], preferred_element_type=F32)

        def pass_on(s):
            for g in range(1, groups):
                ag_copy(sweep, 1, g, s).wait_recv()
                ag_copy(sweep, 2, g, s).start()

        project(0, j)
        for s in range(steps):
            ag_copy(sweep, 0, 0, s).wait_recv()
        project(1, partner)
        pass_on(0)
        for s in range(steps):
            for g in range(1, groups):
                owner = lax.rem(group + groups - g, groups) * 2
                project(2 * g, owner + core, s)
                ag_copy(sweep, 2, g, s).wait_recv()
                project(2 * g + 1, owner + 1 - core, s)
            attend(s)
            if sweep == 0 and s == 0:
                loads[4].wait()
            for g in range(1, groups):
                there = lax.rem(group + g, groups) * 2
                rs_part[sweep, 0, g, s] = head_out(there + 1 - core, s).astype(BF16)
                part_copy(sweep, g, s).start()
                mine[g] = head_out(there + core, s)
            if s < last:
                pass_on(s + 1)
            rs_part[sweep, 0, 0, s] = head_out(partner, s).astype(BF16)
            part_copy(sweep, 0, s).start()
            for g in range(1, groups):
                part_copy(sweep, g, s).wait_recv()
                for c in range(chunks):
                    at = slice(c * piece, (c + 1) * piece)
                    rs_cross[sweep, 0, g - 1, s, c] = (
                        mine[g, at] + rs_part[sweep, 1, g, s, at].astype(F32)
                    ).astype(BF16)
                    cross_copy(sweep, g, s, c).start()
            inc[s] = head_out(j, s)

        sizes = [gaps[s].astype(F32) / (5 * steps * tm) for s in range(steps)]

        def running(s, c):
            at = slice(c * piece, (c + 1) * piece)
            share = inc[s, at] + rs_part[sweep, 1, 0, s, at].astype(F32)
            for g in range(1, groups):
                cross_copy(sweep, g, s, c).wait_recv()
                share = share + rs_cross[sweep, 1, g - 1, s, c].astype(F32)
            total = -sizes[s] * (mods[2, s : s + 1] * share)
            if s > 0:
                total = total + inc[s - 1, at]
            inc[s, at] = total
            return total

        for s in range(last):
            part_copy(sweep, 0, s).wait_recv()
            for c in range(chunks):
                running(s, c)

        @pl.when(link == 0)
        def _():
            chain_recv[sweep] = jnp.zeros_like(chain_recv[sweep])

        part_copy(sweep, 0, last).wait_recv()
        for c in range(chunks):
            ours = running(last, c)

            @pl.when(link > 0)
            def _():
                chain_copy(sweep, c).wait_recv()

            earlier = chain_recv[sweep, c].astype(F32)

            @pl.when(link < pairs - 1)
            def _():
                chain_send[sweep, c] = (earlier + ours).astype(BF16)
                chain_copy(sweep, c).start()

            last_send[sweep, c] = jnp.where(side == 0, earlier + ours, earlier).astype(BF16)
            last_copy(sweep, c).start()
            prefix[c] = earlier
        if sweep == 0:
            @pl.when(k > 0)
            def _():
                start_copy(1).wait_recv()
                start[...] = start_b[1].astype(F32)

            @pl.when(k == 0)
            def _():
                start[...] = traj[0]
        for c in range(chunks):
            at = slice(c * piece, (c + 1) * piece)
            last_copy(sweep, c).wait_recv()
            entry = start[at] + (prefix[c] + last_recv[sweep, c].astype(F32))
            if sweep < ITERS - 1:
                traj[0, at] = entry
                for s in range(1, steps):
                    traj[s, at] = entry + inc[s - 1, at]
            else:
                for s in range(steps):
                    result[s, at] = entry + inc[s, at]

    for d in range(1, tm):
        gap_copy(d).wait_send()

    @pl.when(k == 0)
    def _():
        for d in range(1, tm):
            start_copy(d).wait_send()

    for sweep in range(ITERS):
        for d in range(1, tp):
            stat_copy(sweep, d).wait_send()
        for s in range(steps):
            ag_copy(sweep, 0, 0, s).wait_send()
            for g in range(1, groups):
                ag_copy(sweep, 1, g, s).wait_send()
                ag_copy(sweep, 2, g, s).wait_send()
            for g in range(groups):
                part_copy(sweep, g, s).wait_send()
                for c in range(chunks if g > 0 else 0):
                    cross_copy(sweep, g, s, c).wait_send()
        for c in range(chunks):
            last_copy(sweep, c).wait_send()

        @pl.when(link < pairs - 1)
        def _():
            for c in range(chunks):
                chain_copy(sweep, c).wait_send()


def solution(mesh):
    tm, tp = mesh.shape["tm"], mesh.shape["tp"]
    chunks = 8

    def body(trajectory, offset, step_gaps, qkv_weight, out_weight, mod_weight):
        steps, tok, col = trajectory.shape
        rows, groups = steps * tok, tp // 2
        pieces = (chunks, tok // chunks, col)
        table = level_table(5 * steps * tm)
        qkv = jnp.transpose(qkv_weight, (1, 0, 2))
        mod = jnp.transpose(mod_weight, (1, 0, 2))
        anywhere = pl.BlockSpec(memory_space=pl.ANY)
        smem = pl.BlockSpec(memory_space=pltpu.SMEM)
        vm, dma = pltpu.VMEM, pltpu.SemaphoreType.DMA
        return pl.pallas_call(
            functools.partial(kernel, tm, tp, steps, tok, col),
            out_shape=jax.ShapeDtypeStruct(trajectory.shape, F32),
            in_specs=[smem, smem] + [anywhere] * 5,
            out_specs=pl.BlockSpec(memory_space=pltpu.VMEM),
            scratch_shapes=[
                vm(trajectory.shape, F32),
                vm(table.shape, BF16),
                vm(mod.shape, BF16),
                vm(qkv.shape, BF16),
                vm(out_weight.shape, BF16),
                vm((3, 8, col), F32),
                vm((tm, 8, 128), jnp.int32),
                vm((ITERS, tp, 8, rows), F32),
                vm((ITERS, tp, steps, tok, col), BF16),
                vm((3, rows, col), F32),
                vm((steps, tok, col), BF16),
                vm((ITERS, 2, groups, steps, tok, col), BF16),
                vm((ITERS, 2, max(groups - 1, 1), steps) + pieces, BF16),
                vm((groups, tok, col), F32),
                vm((steps, tok, col), F32),
                vm((ITERS,) + pieces, BF16),
                vm((ITERS,) + pieces, BF16),
                vm((ITERS,) + pieces, BF16),
                vm((ITERS,) + pieces, BF16),
                vm(pieces, F32),
                vm((tok, col), F32),
                vm((2, tok, col), BF16),
                dma((5,)),
                dma((tm,)),
                dma((tm,)),
                dma((ITERS, 2, tp)),
                dma((ITERS, 2, 3, groups, steps)),
                dma((ITERS, 2, groups, steps)),
                dma((ITERS, 2, groups, steps, chunks)),
                dma((ITERS, 4, chunks)),
                dma((tm,)),
                dma,
            ],
            compiler_params=pltpu.CompilerParams(
                collective_id=0, has_side_effects=True, vmem_limit_bytes=62 * 1024 * 1024
            ),
            name="picard",
        )(offset, step_gaps, trajectory, table, mod, qkv, out_weight)

    placed = (
        P("tm", None, "tp"),
        P(),
        P("tm"),
        P(None, None, "tp"),
        P("tp", None),
        P(None, None, "tp"),
    )
    return jax.shard_map(
        body, mesh=mesh, in_specs=placed, out_specs=P("tm", None, "tp"), check_vma=False
    )
```

```python
import functools
import math

import jax
import jax.numpy as jnp
from jax import lax
from jax.experimental import pallas as pl
from jax.experimental.pallas import tpu as pltpu
from jax.sharding import PartitionSpec as P

HD = 128
FREQ = 256
ITERS = 2
F32 = jnp.float32
BF16 = jnp.bfloat16
MESH = pl.DeviceIdType.MESH


def level_table(level_count):
    rows = -(-level_count // 128) * 128
    sigma = 1.0 - jnp.arange(rows, dtype=jnp.int32).astype(F32) / level_count
    half_freq = FREQ // 2
    frequencies = jnp.exp(-math.log(10000.0) * jnp.arange(half_freq, dtype=F32) / half_freq)
    angles = 1000.0 * sigma[:, None] * frequencies[None, :]
    return jnp.concatenate([jnp.cos(angles), jnp.sin(angles)], -1).astype(BF16)


def kernel(
    tm, tp, steps, tok, col,
    offset, gaps, traj_hbm, table_hbm, mod_hbm, qkv_hbm, out_hbm, entry_out, inc_out,
    traj, table, mod_w, qkv_w, out_w, mods,
    gap_buf, stat_buf, normed, acc, attended,
    rs_part, rs_cross, mine, inc, chain_send, chain_recv, last_send,
    last_recv, prefix, start, start_b,
    load_sem, gap_send_sem, gap_recv_sem, stat_sem, ag_sem, rs_sem, cross_sem,
    chain_sem, start_send_sem, start_recv_sem, inc_sem, sums,
):
    k = lax.axis_index("tm")
    j = lax.axis_index("tp")
    rows = steps * tok
    width = tp * col
    chunks = chain_send.shape[1]
    groups = tp // 2
    pairs = tm // 2
    core = lax.rem(j, 2)
    group = lax.div(j, 2)
    side = lax.rem(k, 2)
    link = lax.div(k, 2)
    partner = group * 2 + (1 - core)
    neighbour = link * 2 + (1 - side)

    loads = [
        pltpu.make_async_copy(src, dst, load_sem.at[n])
        for n, (src, dst) in enumerate(
            ((traj_hbm, traj), (table_hbm, table), (mod_hbm, mod_w), (qkv_hbm, qkv_w), (out_hbm, out_w))
        )
    ]
    for load in loads[:3]:
        load.start()

    barrier = pltpu.get_barrier_semaphore()
    for d in range(1, tp):
        pl.semaphore_signal(
            barrier, inc=1, device_id=(k, lax.rem(j + d, tp)), device_id_type=MESH
        )
    for d in range(1, tm):
        pl.semaphore_signal(
            barrier, inc=1, device_id=(lax.rem(k + d, tm), j), device_id_type=MESH
        )

    def send(src, dst, send_sem, recv_sem, to_k, to_j):
        return pltpu.make_async_remote_copy(
            src_ref=src, dst_ref=dst, send_sem=send_sem, recv_sem=recv_sem,
            device_id=(to_k, to_j), device_id_type=MESH,
        )

    own_total = gaps[0]
    for s in range(1, steps):
        own_total = own_total + gaps[s]
    gap_buf[0] = jnp.full((8, 128), own_total, jnp.int32)
    loads[0].wait()
    for load in loads[3:]:
        load.start()

    def row_sums(s, at):
        x = traj[s, at]
        total = jnp.sum(x, -1, keepdims=True)
        squares = jnp.sum(x * x, -1, keepdims=True)
        lane = lax.broadcasted_iota(jnp.int32, (x.shape[0], 128), 1)
        sums[s, at] = jnp.where(lane == 0, total, jnp.where(lane == 1, squares, 0.0))

    def turn_sums(sweep):
        stat_buf[sweep, 0] = jnp.transpose(sums[...].reshape(rows, 128))[0:8]

    for s in range(steps):
        row_sums(s, slice(0, tok))
    turn_sums(0)
    start_b[0] = traj[0].astype(BF16)
    pl.semaphore_wait(barrier, tp - 1 + tm - 1)

    def stat_copy(sweep, d):
        return send(
            stat_buf.at[sweep, 0], stat_buf.at[sweep, d],
            stat_sem.at[sweep, 0, d], stat_sem.at[sweep, 1, d], k, lax.rem(j + d, tp),
        )

    def gap_copy(d):
        return send(
            gap_buf.at[0], gap_buf.at[d], gap_send_sem.at[d], gap_recv_sem.at[d],
            lax.rem(k + d, tm), j,
        )

    def start_copy(d):
        return send(start_b.at[0], start_b.at[1], start_send_sem.at[d], start_recv_sem, d, j)

    for d in range(1, tm):
        gap_copy(d).start()
    for d in range(1, tp):
        stat_copy(0, d).start()

    @pl.when(k == 0)
    def _():
        for d in range(1, tm):
            start_copy(d).start()

    before = jnp.full((8, 128), offset[0], jnp.int32)
    for d in range(1, tm):
        gap_copy(d).wait_recv()
        before = before + jnp.where(k >= d, gap_buf[d], 0)
    row = lax.broadcasted_iota(jnp.int32, (8, 128), 0)
    for s in range(steps):
        before = before + jnp.where(row > s, gaps[s], 0)
    loads[1].wait()
    table_rows = table.shape[0]
    levels = jnp.concatenate([before] * (table_rows // 128), -1)
    pick = (lax.broadcasted_iota(jnp.int32, (8, table_rows), 1) == levels).astype(F32).astype(BF16)
    embed = jnp.dot(pick, table[...], preferred_element_type=F32).astype(BF16)
    loads[2].wait()
    for part in range(3):
        mods[part] = jnp.dot(embed, mod_w[part], preferred_element_type=F32)

    def ag_copy(sweep, kind, g, s):
        sems = (ag_sem.at[sweep, 0, kind, g, s], ag_sem.at[sweep, 1, kind, g, s])
        if kind == 0:
            return send(normed.at[sweep, 0, s], normed.at[sweep, 1, s], *sems, k, partner)
        if kind == 1:
            there = lax.rem(group + g, groups) * 2 + core
            return send(normed.at[sweep, 0, s], normed.at[sweep, 2 * g, s], *sems, k, there)
        return send(normed.at[sweep, 2 * g, s], normed.at[sweep, 2 * g + 1, s], *sems, k, partner)

    def part_copy(sweep, g, s):
        return send(
            rs_part.at[sweep, 0, g, s], rs_part.at[sweep, 1, g, s],
            rs_sem.at[sweep, 0, g, s], rs_sem.at[sweep, 1, g, s], k, partner,
        )

    def cross_copy(sweep, g, s, c):
        there = lax.rem(group + g, groups) * 2 + core
        return send(
            rs_cross.at[sweep, 0, g - 1, s, c], rs_cross.at[sweep, 1, g - 1, s, c],
            cross_sem.at[sweep, 0, g, s, c], cross_sem.at[sweep, 1, g, s, c], k, there,
        )

    def last_copy(sweep, c):
        return send(
            last_send.at[sweep, c], last_recv.at[sweep, c],
            chain_sem.at[sweep, 2, c], chain_sem.at[sweep, 3, c], neighbour, j,
        )

    def chain_copy(sweep, c):
        return send(
            chain_send.at[sweep, c], chain_recv.at[sweep, c],
            chain_sem.at[sweep, 0, c], chain_sem.at[sweep, 1, c], lax.rem(k + 2, tm), j,
        )

    def inc_copy(n):
        return pltpu.make_async_copy(inc.at[n], inc_out.at[n], inc_sem.at[n])

    piece = tok // chunks
    last = steps - 1

    for sweep in range(ITERS):
        if sweep > 0:
            turn_sums(sweep)
            for d in range(1, tp):
                stat_copy(sweep, d).start()
        stats = stat_buf[sweep, 0]
        for d in range(1, tp):
            stat_copy(sweep, d).wait_recv()
            stats = stats + stat_buf[sweep, d]
        stats = jnp.transpose(
            jnp.concatenate([stats, jnp.zeros((120, rows), F32)], 0)
        )
        row_mean = stats[:, 0:1] / width
        variance = stats[:, 1:2] / width - row_mean * row_mean
        inv_std = lax.rsqrt(variance + 1e-06)
        for s in range(steps):
            part = slice(s * tok, (s + 1) * tok)
            normed[sweep, 0, s] = (
                (traj[s] - row_mean[part]) * inv_std[part] * (1.0 + mods[1, s : s + 1])
                + mods[0, s : s + 1]
            ).astype(BF16)
            for g in range(1, groups):
                ag_copy(sweep, 1, g, s).start()
            ag_copy(sweep, 0, 0, s).start()

        if sweep == 0:
            loads[3].wait()

        def project(slot, owner, s=None):
            block = normed[sweep, slot].reshape(rows, col) if s is None else normed[sweep, slot, s]
            into = slice(0, rows) if s is None else slice(s * tok, (s + 1) * tok)
            at = pl.multiple_of(owner * col, col)

            def one(part, carry):
                product = jnp.dot(block, qkv_w[part, pl.ds(at, col), :], preferred_element_type=F32)
                if slot == 0:
                    acc[part, into] = product
                else:
                    acc[part, into] = acc[part, into] + product
                return carry

            lax.fori_loop(0, 3, one, 0)

        def attend(s):
            at = slice(s * tok, (s + 1) * tok)
            heads = [slice(head * HD, (head + 1) * HD) for head in range(col // HD)]
            scores = jnp.concatenate(
                [
                    lax.dot_general(
                        acc[0, at, lanes].astype(BF16), acc[1, at, lanes].astype(BF16),
                        (((1,), (1,)), ((), ())), preferred_element_type=F32,
                    )
                    for lanes in heads
                ],
                0,
            ) * (1.0 / math.sqrt(HD))
            weights_exp = jnp.exp(scores - jnp.max(scores, -1, keepdims=True))
            probs = (weights_exp / jnp.sum(weights_exp, -1, keepdims=True)).astype(BF16)
            for head, lanes in enumerate(heads):
                attended[s, :, lanes] = jnp.dot(
                    probs[head * tok : (head + 1) * tok], acc[2, at, lanes].astype(BF16),
                    preferred_element_type=F32,
                ).astype(BF16)

        def head_out(dest, s):
            at = pl.ds(pl.multiple_of(dest * col, col), col)
            return jnp.dot(attended[s], out_w[:, at], preferred_element_type=F32)

        def pass_on(s):
            for g in range(1, groups):
                ag_copy(sweep, 1, g, s).wait_recv()
                ag_copy(sweep, 2, g, s).start()

        project(0, j)
        for s in range(steps):
            ag_copy(sweep, 0, 0, s).wait_recv()
        project(1, partner)
        pass_on(0)
        for s in range(steps):
            for g in range(1, groups):
                owner = lax.rem(group + groups - g, groups) * 2
                project(2 * g, owner + core, s)
                ag_copy(sweep, 2, g, s).wait_recv()
                project(2 * g + 1, owner + 1 - core, s)
            attend(s)
            if sweep == 0 and s == 0:
                loads[4].wait()
            for g in range(1, groups):
                there = lax.rem(group + g, groups) * 2
                rs_part[sweep, 0, g, s] = head_out(there + 1 - core, s).astype(BF16)
                part_copy(sweep, g, s).start()
                mine[g] = head_out(there + core, s)
            if s < last:
                pass_on(s + 1)
            rs_part[sweep, 0, 0, s] = head_out(partner, s).astype(BF16)
            part_copy(sweep, 0, s).start()
            for g in range(1, groups):
                part_copy(sweep, g, s).wait_recv()
                for c in range(chunks):
                    at = slice(c * piece, (c + 1) * piece)
                    rs_cross[sweep, 0, g - 1, s, c] = (
                        mine[g, at] + rs_part[sweep, 1, g, s, at].astype(F32)
                    ).astype(BF16)
                    cross_copy(sweep, g, s, c).start()
            inc[s] = head_out(j, s)

        sizes = [gaps[s].astype(F32) / (5 * steps * tm) for s in range(steps)]

        def running(s, c):
            at = slice(c * piece, (c + 1) * piece)
            share = inc[s, at] + rs_part[sweep, 1, 0, s, at].astype(F32)
            for g in range(1, groups):
                cross_copy(sweep, g, s, c).wait_recv()
                share = share + rs_cross[sweep, 1, g - 1, s, c].astype(F32)
            total = -sizes[s] * (mods[2, s : s + 1] * share)
            if s > 0:
                total = total + inc[s - 1, at]
            inc[s, at] = total
            return total

        for s in range(last):
            part_copy(sweep, 0, s).wait_recv()
            for c in range(chunks):
                running(s, c)

        @pl.when(link == 0)
        def _():
            chain_recv[sweep] = jnp.zeros_like(chain_recv[sweep])

        part_copy(sweep, 0, last).wait_recv()
        for c in range(chunks):
            ours = running(last, c)

            @pl.when(link > 0)
            def _():
                chain_copy(sweep, c).wait_recv()

            earlier = chain_recv[sweep, c].astype(F32)

            @pl.when(link < pairs - 1)
            def _():
                chain_send[sweep, c] = (earlier + ours).astype(BF16)
                chain_copy(sweep, c).start()

            last_send[sweep, c] = jnp.where(side == 0, earlier + ours, earlier).astype(BF16)
            last_copy(sweep, c).start()
            prefix[c] = earlier
        if sweep == ITERS - 1:
            for n in range(steps):
                inc_copy(n).start()
        if sweep == 0:
            @pl.when(k > 0)
            def _():
                start_copy(1).wait_recv()
                start[...] = start_b[1].astype(F32)

            @pl.when(k == 0)
            def _():
                start[...] = traj[0]
        for c in range(chunks):
            at = slice(c * piece, (c + 1) * piece)
            last_copy(sweep, c).wait_recv()
            entry = start[at] + (prefix[c] + last_recv[sweep, c].astype(F32))
            if sweep < ITERS - 1:
                traj[0, at] = entry
                for s in range(1, steps):
                    traj[s, at] = entry + inc[s - 1, at]
                for s in range(steps):
                    row_sums(s, at)
            else:
                entry_out[at] = entry

    for n in range(steps):
        inc_copy(n).wait()
    for d in range(1, tm):
        gap_copy(d).wait_send()

    @pl.when(k == 0)
    def _():
        for d in range(1, tm):
            start_copy(d).wait_send()

    for sweep in range(ITERS):
        for d in range(1, tp):
            stat_copy(sweep, d).wait_send()
        for s in range(steps):
            ag_copy(sweep, 0, 0, s).wait_send()
            for g in range(1, groups):
                ag_copy(sweep, 1, g, s).wait_send()
                ag_copy(sweep, 2, g, s).wait_send()
            for g in range(groups):
                part_copy(sweep, g, s).wait_send()
                for c in range(chunks if g > 0 else 0):
                    cross_copy(sweep, g, s, c).wait_send()
        for c in range(chunks):
            last_copy(sweep, c).wait_send()

        @pl.when(link < pairs - 1)
        def _():
            for c in range(chunks):
                chain_copy(sweep, c).wait_send()


def solution(mesh):
    tm, tp = mesh.shape["tm"], mesh.shape["tp"]
    chunks = 8

    def body(trajectory, offset, step_gaps, qkv_weight, out_weight, mod_weight):
        steps, tok, col = trajectory.shape
        rows, groups = steps * tok, tp // 2
        pieces = (chunks, tok // chunks, col)
        table = level_table(5 * steps * tm)
        qkv = jnp.transpose(qkv_weight, (1, 0, 2))
        mod = jnp.transpose(mod_weight, (1, 0, 2))
        anywhere = pl.BlockSpec(memory_space=pl.ANY)
        smem = pl.BlockSpec(memory_space=pltpu.SMEM)
        vm, dma = pltpu.VMEM, pltpu.SemaphoreType.DMA
        entry, increments = pl.pallas_call(
            functools.partial(kernel, tm, tp, steps, tok, col),
            out_shape=(
                jax.ShapeDtypeStruct((tok, col), F32),
                jax.ShapeDtypeStruct(trajectory.shape, F32),
            ),
            in_specs=[smem, smem] + [anywhere] * 5,
            out_specs=(pl.BlockSpec(memory_space=pltpu.VMEM), anywhere),
            scratch_shapes=[
                vm(trajectory.shape, F32),
                vm(table.shape, BF16),
                vm(mod.shape, BF16),
                vm(qkv.shape, BF16),
                vm(out_weight.shape, BF16),
                vm((3, 8, col), F32),
                vm((tm, 8, 128), jnp.int32),
                vm((ITERS, tp, 8, rows), F32),
                vm((ITERS, tp, steps, tok, col), BF16),
                vm((3, rows, col), F32),
                vm((steps, tok, col), BF16),
                vm((ITERS, 2, groups, steps, tok, col), BF16),
                vm((ITERS, 2, max(groups - 1, 1), steps) + pieces, BF16),
                vm((groups, tok, col), F32),
                vm((steps, tok, col), F32),
                vm((ITERS,) + pieces, BF16),
                vm((ITERS,) + pieces, BF16),
                vm((ITERS,) + pieces, BF16),
                vm((ITERS,) + pieces, BF16),
                vm(pieces, F32),
                vm((tok, col), F32),
                vm((2, tok, col), BF16),
                dma((5,)),
                dma((tm,)),
                dma((tm,)),
                dma((ITERS, 2, tp)),
                dma((ITERS, 2, 3, groups, steps)),
                dma((ITERS, 2, groups, steps)),
                dma((ITERS, 2, groups, steps, chunks)),
                dma((ITERS, 4, chunks)),
                dma((tm,)),
                dma,
                dma((steps,)),
                vm((steps, tok, 128), F32),
            ],
            compiler_params=pltpu.CompilerParams(
                collective_id=0, has_side_effects=True, vmem_limit_bytes=62 * 1024 * 1024
            ),
            name="picard",
        )(offset, step_gaps, trajectory, table, mod, qkv, out_weight)
        return entry[None] + increments

    placed = (
        P("tm", None, "tp"),
        P(),
        P("tm"),
        P(None, None, "tp"),
        P("tp", None),
        P(None, None, "tp"),
    )
    return jax.shard_map(
        body, mesh=mesh, in_specs=placed, out_specs=P("tm", None, "tp"), check_vma=False
    )
```

```python
import functools
import math

import jax
import jax.numpy as jnp
from jax import lax
from jax.experimental import pallas as pl
from jax.experimental.pallas import tpu as pltpu
from jax.sharding import PartitionSpec as P

HD = 128
FREQ = 256
ITERS = 2
F32 = jnp.float32
BF16 = jnp.bfloat16
MESH = pl.DeviceIdType.MESH


def level_table(level_count):
    rows = -(-level_count // 128) * 128
    sigma = 1.0 - jnp.arange(rows, dtype=jnp.int32).astype(F32) / level_count
    half_freq = FREQ // 2
    frequencies = jnp.exp(-math.log(10000.0) * jnp.arange(half_freq, dtype=F32) / half_freq)
    angles = 1000.0 * sigma[:, None] * frequencies[None, :]
    return jnp.concatenate([jnp.cos(angles), jnp.sin(angles)], -1).astype(BF16)


def kernel(
    tm, tp, steps, tok, col,
    offset, gaps, traj_hbm, table_hbm, mod_hbm, qkv_hbm, out_hbm, entry_out, inc_out,
    traj, table, mod_w, qkv_w, out_w, mods,
    gap_buf, stat_buf, normed, acc, attended,
    rs_part, rs_cross, mine, inc, chain_send, chain_recv, last_send,
    last_recv, prefix, start, start_b,
    load_sem, gap_send_sem, gap_recv_sem, stat_sem, ag_sem, rs_sem, cross_sem,
    chain_sem, start_send_sem, start_recv_sem, inc_sem, sums,
):
    k = lax.axis_index("tm")
    j = lax.axis_index("tp")
    rows = steps * tok
    width = tp * col
    chunks = chain_send.shape[1]
    groups = tp // 2
    pairs = tm // 2
    core = lax.rem(j, 2)
    group = lax.div(j, 2)
    side = lax.rem(k, 2)
    link = lax.div(k, 2)
    partner = group * 2 + (1 - core)
    neighbour = link * 2 + (1 - side)

    loads = [
        pltpu.make_async_copy(src, dst, load_sem.at[n])
        for n, (src, dst) in enumerate(
            ((traj_hbm, traj), (table_hbm, table), (mod_hbm, mod_w), (qkv_hbm, qkv_w), (out_hbm, out_w))
        )
    ]
    for load in loads[:3]:
        load.start()

    barrier = pltpu.get_barrier_semaphore()
    for d in range(1, tp):
        pl.semaphore_signal(
            barrier, inc=1, device_id=(k, lax.rem(j + d, tp)), device_id_type=MESH
        )
    for d in range(1, tm):
        pl.semaphore_signal(
            barrier, inc=1, device_id=(lax.rem(k + d, tm), j), device_id_type=MESH
        )

    def send(src, dst, send_sem, recv_sem, to_k, to_j):
        return pltpu.make_async_remote_copy(
            src_ref=src, dst_ref=dst, send_sem=send_sem, recv_sem=recv_sem,
            device_id=(to_k, to_j), device_id_type=MESH,
        )

    own_total = gaps[0]
    for s in range(1, steps):
        own_total = own_total + gaps[s]
    gap_buf[0] = jnp.full((8, 128), own_total, jnp.int32)
    loads[0].wait()
    for load in loads[3:]:
        load.start()

    def row_sums(s, at):
        x = traj[s, at]
        total = jnp.sum(x, -1, keepdims=True)
        squares = jnp.sum(x * x, -1, keepdims=True)
        lane = lax.broadcasted_iota(jnp.int32, (x.shape[0], 128), 1)
        sums[s, at] = jnp.where(lane == 0, total, jnp.where(lane == 1, squares, 0.0))

    def turn_sums(sweep):
        stat_buf[sweep, 0] = jnp.transpose(sums[...].reshape(rows, 128))[0:8]

    for s in range(steps):
        row_sums(s, slice(0, tok))
    turn_sums(0)
    start_b[0] = traj[0].astype(BF16)
    pl.semaphore_wait(barrier, tp - 1 + tm - 1)

    def stat_copy(sweep, d):
        return send(
            stat_buf.at[sweep, 0], stat_buf.at[sweep, d],
            stat_sem.at[sweep, 0, d], stat_sem.at[sweep, 1, d], k, lax.rem(j + d, tp),
        )

    def gap_copy(d):
        return send(
            gap_buf.at[0], gap_buf.at[d], gap_send_sem.at[d], gap_recv_sem.at[d],
            lax.rem(k + d, tm), j,
        )

    def start_copy(d):
        return send(start_b.at[0], start_b.at[1], start_send_sem.at[d], start_recv_sem, d, j)

    for d in range(1, tm):
        gap_copy(d).start()
    for d in range(1, tp):
        stat_copy(0, d).start()

    @pl.when(k == 0)
    def _():
        for d in range(1, tm):
            start_copy(d).start()

    before = jnp.full((8, 128), offset[0], jnp.int32)
    for d in range(1, tm):
        gap_copy(d).wait_recv()
        before = before + jnp.where(k >= d, gap_buf[d], 0)
    row = lax.broadcasted_iota(jnp.int32, (8, 128), 0)
    for s in range(steps):
        before = before + jnp.where(row > s, gaps[s], 0)
    loads[1].wait()
    table_rows = table.shape[0]
    levels = jnp.concatenate([before] * (table_rows // 128), -1)
    pick = (lax.broadcasted_iota(jnp.int32, (8, table_rows), 1) == levels).astype(F32).astype(BF16)
    embed = jnp.dot(pick, table[...], preferred_element_type=F32).astype(BF16)
    loads[2].wait()
    for part in range(3):
        mods[part] = jnp.dot(embed, mod_w[part], preferred_element_type=F32)

    def ag_copy(sweep, kind, g, s):
        sems = (ag_sem.at[sweep, 0, kind, g, s], ag_sem.at[sweep, 1, kind, g, s])
        if kind == 0:
            return send(normed.at[sweep, 0, s], normed.at[sweep, 1, s], *sems, k, partner)
        if kind == 1:
            there = lax.rem(group + g, groups) * 2 + core
            return send(normed.at[sweep, 0, s], normed.at[sweep, 2 * g, s], *sems, k, there)
        return send(normed.at[sweep, 2 * g, s], normed.at[sweep, 2 * g + 1, s], *sems, k, partner)

    def part_copy(sweep, g, s):
        return send(
            rs_part.at[sweep, 0, g, s], rs_part.at[sweep, 1, g, s],
            rs_sem.at[sweep, 0, g, s], rs_sem.at[sweep, 1, g, s], k, partner,
        )

    def cross_copy(sweep, g, s, c):
        there = lax.rem(group + g, groups) * 2 + core
        return send(
            rs_cross.at[sweep, 0, g - 1, s, c], rs_cross.at[sweep, 1, g - 1, s, c],
            cross_sem.at[sweep, 0, g, s, c], cross_sem.at[sweep, 1, g, s, c], k, there,
        )

    def last_copy(sweep, c):
        return send(
            last_send.at[sweep, c], last_recv.at[sweep, c],
            chain_sem.at[sweep, 2, c], chain_sem.at[sweep, 3, c], neighbour, j,
        )

    def chain_copy(sweep, c):
        return send(
            chain_send.at[sweep, c], chain_recv.at[sweep, c],
            chain_sem.at[sweep, 0, c], chain_sem.at[sweep, 1, c], lax.rem(k + 2, tm), j,
        )

    def inc_copy(n):
        return pltpu.make_async_copy(inc.at[n], inc_out.at[n], inc_sem.at[n])

    piece = tok // chunks
    last = steps - 1

    for sweep in range(ITERS):
        if sweep > 0:
            turn_sums(sweep)
            for d in range(1, tp):
                stat_copy(sweep, d).start()
        stats = stat_buf[sweep, 0]
        for d in range(1, tp):
            stat_copy(sweep, d).wait_recv()
            stats = stats + stat_buf[sweep, d]
        stats = jnp.transpose(
            jnp.concatenate([stats, jnp.zeros((120, rows), F32)], 0)
        )
        row_mean = stats[:, 0:1] / width
        variance = stats[:, 1:2] / width - row_mean * row_mean
        inv_std = lax.rsqrt(variance + 1e-06)
        for s in range(steps):
            part = slice(s * tok, (s + 1) * tok)
            normed[sweep, 0, s] = (
                (traj[s] - row_mean[part]) * inv_std[part] * (1.0 + mods[1, s : s + 1])
                + mods[0, s : s + 1]
            ).astype(BF16)
            for g in range(1, groups):
                ag_copy(sweep, 1, g, s).start()
            ag_copy(sweep, 0, 0, s).start()

        if sweep == 0:
            loads[3].wait()

        def project(slot, owner, s=None):
            block = normed[sweep, slot].reshape(rows, col) if s is None else normed[sweep, slot, s]
            into = slice(0, rows) if s is None else slice(s * tok, (s + 1) * tok)
            at = pl.multiple_of(owner * col, col)

            def one(part, carry):
                product = jnp.dot(block, qkv_w[part, pl.ds(at, col), :], preferred_element_type=F32)
                if slot == 0:
                    acc[part, into] = product
                else:
                    acc[part, into] = acc[part, into] + product
                return carry

            lax.fori_loop(0, 3, one, 0)

        def attend(s):
            at = slice(s * tok, (s + 1) * tok)
            heads = [slice(head * HD, (head + 1) * HD) for head in range(col // HD)]
            scores = jnp.concatenate(
                [
                    lax.dot_general(
                        acc[0, at, lanes].astype(BF16), acc[1, at, lanes].astype(BF16),
                        (((1,), (1,)), ((), ())), preferred_element_type=F32,
                    )
                    for lanes in heads
                ],
                0,
            ) * (1.0 / math.sqrt(HD))
            weights_exp = jnp.exp(scores - jnp.max(scores, -1, keepdims=True))
            probs = (weights_exp / jnp.sum(weights_exp, -1, keepdims=True)).astype(BF16)
            for head, lanes in enumerate(heads):
                attended[s, :, lanes] = jnp.dot(
                    probs[head * tok : (head + 1) * tok], acc[2, at, lanes].astype(BF16),
                    preferred_element_type=F32,
                ).astype(BF16)

        def head_out(dest, s):
            at = pl.ds(pl.multiple_of(dest * col, col), col)
            return jnp.dot(attended[s], out_w[:, at], preferred_element_type=F32)

        def pass_on(s):
            for g in range(1, groups):
                ag_copy(sweep, 1, g, s).wait_recv()
                ag_copy(sweep, 2, g, s).start()

        project(0, j)
        for s in range(steps):
            ag_copy(sweep, 0, 0, s).wait_recv()
        project(1, partner)
        pass_on(0)
        for s in range(steps):
            for g in range(1, groups):
                owner = lax.rem(group + groups - g, groups) * 2
                project(2 * g, owner + core, s)
                ag_copy(sweep, 2, g, s).wait_recv()
                project(2 * g + 1, owner + 1 - core, s)
            attend(s)
            if sweep == 0 and s == 0:
                loads[4].wait()
            for g in range(1, groups):
                there = lax.rem(group + g, groups) * 2
                rs_part[sweep, 0, g, s] = head_out(there + 1 - core, s).astype(BF16)
                part_copy(sweep, g, s).start()
                mine[g] = head_out(there + core, s)
            if s < last:
                pass_on(s + 1)
            rs_part[sweep, 0, 0, s] = head_out(partner, s).astype(BF16)
            part_copy(sweep, 0, s).start()
            for g in range(1, groups):
                part_copy(sweep, g, s).wait_recv()
                for c in range(chunks):
                    at = slice(c * piece, (c + 1) * piece)
                    rs_cross[sweep, 0, g - 1, s, c] = (
                        mine[g, at] + rs_part[sweep, 1, g, s, at].astype(F32)
                    ).astype(BF16)
                    cross_copy(sweep, g, s, c).start()
            inc[s] = head_out(j, s)

        sizes = [gaps[s].astype(F32) / (5 * steps * tm) for s in range(steps)]

        def running(s, c):
            at = slice(c * piece, (c + 1) * piece)
            share = inc[s, at] + rs_part[sweep, 1, 0, s, at].astype(F32)
            for g in range(1, groups):
                cross_copy(sweep, g, s, c).wait_recv()
                share = share + rs_cross[sweep, 1, g - 1, s, c].astype(F32)
            total = -sizes[s] * (mods[2, s : s + 1] * share)
            if s > 0:
                total = total + inc[s - 1, at]
            inc[s, at] = total
            return total

        for s in range(last):
            part_copy(sweep, 0, s).wait_recv()
            for c in range(chunks):
                running(s, c)

        @pl.when(link == 0)
        def _():
            chain_recv[sweep] = jnp.zeros_like(chain_recv[sweep])

        part_copy(sweep, 0, last).wait_recv()
        for c in range(chunks):
            ours = running(last, c)

            @pl.when(link > 0)
            def _():
                chain_copy(sweep, c).wait_recv()

            earlier = chain_recv[sweep, c].astype(F32)

            @pl.when(link < pairs - 1)
            def _():
                chain_send[sweep, c] = (earlier + ours).astype(BF16)
                chain_copy(sweep, c).start()

            last_send[sweep, c] = jnp.where(side == 0, earlier + ours, earlier).astype(BF16)
            last_copy(sweep, c).start()
            prefix[c] = earlier
        if sweep == ITERS - 1:
            for n in range(steps):
                inc_copy(n).start()
        if sweep == 0:
            @pl.when(k > 0)
            def _():
                start_copy(1).wait_recv()
                start[...] = start_b[1].astype(F32)

            @pl.when(k == 0)
            def _():
                start[...] = traj[0]
        for c in range(chunks):
            at = slice(c * piece, (c + 1) * piece)
            last_copy(sweep, c).wait_recv()
            entry = start[at] + (prefix[c] + last_recv[sweep, c].astype(F32))
            if sweep < ITERS - 1:
                traj[0, at] = entry
                for s in range(1, steps):
                    traj[s, at] = entry + inc[s - 1, at]
                for s in range(steps):
                    row_sums(s, at)
            else:
                entry_out[at] = entry

    for n in range(steps):
        inc_copy(n).wait()
    for d in range(1, tm):
        gap_copy(d).wait_send()

    @pl.when(k == 0)
    def _():
        for d in range(1, tm):
            start_copy(d).wait_send()

    for sweep in range(ITERS):
        for d in range(1, tp):
            stat_copy(sweep, d).wait_send()
        for s in range(steps):
            ag_copy(sweep, 0, 0, s).wait_send()
            for g in range(1, groups):
                ag_copy(sweep, 1, g, s).wait_send()
                ag_copy(sweep, 2, g, s).wait_send()
            for g in range(groups):
                part_copy(sweep, g, s).wait_send()
                for c in range(chunks if g > 0 else 0):
                    cross_copy(sweep, g, s, c).wait_send()
        for c in range(chunks):
            last_copy(sweep, c).wait_send()

        @pl.when(link < pairs - 1)
        def _():
            for c in range(chunks):
                chain_copy(sweep, c).wait_send()


def solution(mesh):
    tm, tp = mesh.shape["tm"], mesh.shape["tp"]
    chunks = 8

    def body(trajectory, offset, step_gaps, qkv_weight, out_weight, mod_weight):
        steps, tok, col = trajectory.shape
        rows, groups = steps * tok, tp // 2
        pieces = (chunks, tok // chunks, col)
        table = level_table(5 * steps * tm)
        qkv = jnp.transpose(qkv_weight, (1, 0, 2))
        mod = jnp.transpose(mod_weight, (1, 0, 2))
        anywhere = pl.BlockSpec(memory_space=pl.ANY)
        smem = pl.BlockSpec(memory_space=pltpu.SMEM)
        vm, dma = pltpu.VMEM, pltpu.SemaphoreType.DMA
        entry, increments = pl.pallas_call(
            functools.partial(kernel, tm, tp, steps, tok, col),
            out_shape=(
                jax.ShapeDtypeStruct((tok, col), F32),
                jax.ShapeDtypeStruct(trajectory.shape, F32),
            ),
            in_specs=[smem, smem] + [anywhere] * 5,
            out_specs=(pl.BlockSpec(memory_space=pltpu.VMEM), anywhere),
            scratch_shapes=[
                vm(trajectory.shape, F32),
                vm(table.shape, BF16),
                vm(mod.shape, BF16),
                vm(qkv.shape, BF16),
                vm(out_weight.shape, BF16),
                vm((3, 8, col), F32),
                vm((tm, 8, 128), jnp.int32),
                vm((ITERS, tp, 8, rows), F32),
                vm((ITERS, tp, steps, tok, col), BF16),
                vm((3, rows, col), F32),
                vm((steps, tok, col), BF16),
                vm((ITERS, 2, groups, steps, tok, col), BF16),
                vm((ITERS, 2, max(groups - 1, 1), steps) + pieces, BF16),
                vm((groups, tok, col), F32),
                vm((steps, tok, col), F32),
                vm((ITERS,) + pieces, BF16),
                vm((ITERS,) + pieces, BF16),
                vm((ITERS,) + pieces, BF16),
                vm((ITERS,) + pieces, BF16),
                vm(pieces, F32),
                vm((tok, col), F32),
                vm((2, tok, col), BF16),
                dma((5,)),
                dma((tm,)),
                dma((tm,)),
                dma((ITERS, 2, tp)),
                dma((ITERS, 2, 3, groups, steps)),
                dma((ITERS, 2, groups, steps)),
                dma((ITERS, 2, groups, steps, chunks)),
                dma((ITERS, 4, chunks)),
                dma((tm,)),
                dma,
                dma((steps,)),
                vm((steps, tok, 128), F32),
            ],
            compiler_params=pltpu.CompilerParams(
                collective_id=0, has_side_effects=True, vmem_limit_bytes=51 * 1024 * 1024
            ),
            name="picard",
        )(offset, step_gaps, trajectory, table, mod, qkv, out_weight)
        return entry[None] + increments

    placed = (
        P("tm", None, "tp"),
        P(),
        P("tm"),
        P(None, None, "tp"),
        P("tp", None),
        P(None, None, "tp"),
    )
    return jax.shard_map(
        body, mesh=mesh, in_specs=placed, out_specs=P("tm", None, "tp"), check_vma=False
    )
```
